32 devices in a mesh: rep: 1 (over z), data: 4 (over y), expert: 8 (over x, core).
Axes of the slice: x: 4, y: 4, z: 1, core: 2. Of those that a mesh axis runs over, the one named last changes fastest.
The devices are a block of a 4x4x8 slice.
Arguments:
- tok_in: bfloat16 [65536, 768], P(('rep', 'expert', 'data'))
- expert_idx: int32 [65536, 4], P(('rep', 'expert', 'data'))
- gate_wt: float32 [65536, 4], P(('rep', 'expert', 'data'))
- w_gate: bfloat16 [16, 768, 1344], P('expert', 'data')
- w_up: bfloat16 [16, 768, 1344], P('expert', 'data')
- w_down: bfloat16 [16, 1344, 768], P('expert', None, 'data')
- grad_out: bfloat16 [65536, 768], P(('rep', 'expert', 'data'))
Outputs:
- output 1: bfloat16 [65536, 768], P(('rep', 'expert', 'data'))
- output 2: bfloat16 [65536, 768], P(('rep', 'expert', 'data'))
- output 3: float32 [16, 768, 1344], P(('rep', 'expert'), 'data')
- output 4: float32 [16, 768, 1344], P(('rep', 'expert'), 'data')
- output 5: float32 [16, 1344, 768], P(('rep', 'expert'), None, 'data')
All inputs are finite; a program needn't handle non-finite values.
Results may differ from the reference program's by a relative error of at most 0.001.
Values are sent between devices in bfloat16 or wider.
A program may use at most 768 MiB of HBM per device.

```python
import jax
import jax.numpy as jnp
from jax import lax

TOKENS = 2048
HIDDEN = 768
FFN_DIM = 1344
EXPERTS = 16
TOP_K = 4
EP_SIZE = 8
DP_SIZE = 4

GROUP_DEVS = EP_SIZE * DP_SIZE
PART_TOKENS = GROUP_DEVS * TOKENS
CAPACITY = (5 * TOP_K * TOKENS + 4 * EXPERTS - 1) // (4 * EXPERTS)
HOT_COUNT = max(1, EXPERTS // 8)
TOTAL_ROWS = EXPERTS * GROUP_DEVS * CAPACITY


def draw_routing(route_key, hot_key):
    expert_perm = jax.random.permutation(hot_key, EXPERTS)
    hot_bonus = jnp.where(expert_perm < HOT_COUNT, 6554, 0)
    local_tok = jnp.arange(PART_TOKENS) % TOKENS
    forced = (local_tok[:, None] < CAPACITY) & (expert_perm[None, :] == 0)
    scores = jax.random.randint(route_key, (PART_TOKENS, EXPERTS), 0, 65536, dtype=jnp.int32)
    scores = scores + hot_bonus[None, :] + jnp.where(forced, 131072, 0)
    keyed_scores = scores * EXPERTS + jnp.arange(EXPERTS, dtype=jnp.int32)[None, :]
    return lax.top_k(keyed_scores, TOP_K)[1].astype(jnp.int32)


def setup_inputs(seed: int = 0, part: int = 0) -> dict:
    shared_keys = jax.random.split(jax.random.key(seed), 3)
    part_keys = jax.random.split(jax.random.fold_in(jax.random.key(seed + 1), part), 5)
    tok_in = jax.random.normal(part_keys[0], (PART_TOKENS, HIDDEN), jnp.float32).astype(jnp.bfloat16)
    expert_idx = draw_routing(part_keys[1], part_keys[2])
    gate_wt = jax.random.uniform(part_keys[3], (PART_TOKENS, TOP_K), jnp.float32, 0.5, 1.5) * TOP_K ** -0.5
    w_gate = (jax.random.normal(shared_keys[0], (EXPERTS, HIDDEN, FFN_DIM), jnp.float32) * HIDDEN ** -0.5).astype(jnp.bfloat16)
    w_up = (jax.random.normal(shared_keys[1], (EXPERTS, HIDDEN, FFN_DIM), jnp.float32) * HIDDEN ** -0.5).astype(jnp.bfloat16)
    w_down = (jax.random.normal(shared_keys[2], (EXPERTS, FFN_DIM, HIDDEN), jnp.float32) * (1.6 * FFN_DIM ** -0.5)).astype(jnp.bfloat16)
    grad_out = jax.random.normal(part_keys[4], (PART_TOKENS, HIDDEN), jnp.float32).astype(jnp.bfloat16)
    return dict(tok_in=tok_in, expert_idx=expert_idx, gate_wt=gate_wt, w_gate=w_gate, w_up=w_up, w_down=w_down, grad_out=grad_out)


def expert_step(operands):
    exp_rows, exp_cots, gate_mat, up_mat, down_mat = operands
    pre_gate = jnp.dot(exp_rows, gate_mat, preferred_element_type=jnp.float32)
    pre_up = jnp.dot(exp_rows, up_mat, preferred_element_type=jnp.float32)
    sig_gate = jax.nn.sigmoid(pre_gate)
    silu_gate = pre_gate * sig_gate
    hid_act = (silu_gate * pre_up).astype(jnp.bfloat16)
    exp_out = jnp.dot(hid_act, down_mat, preferred_element_type=jnp.float32).astype(jnp.bfloat16)
    grad_down = jnp.dot(hid_act.T, exp_cots, preferred_element_type=jnp.float32)
    grad_hid = jnp.dot(exp_cots, down_mat.T, preferred_element_type=jnp.float32)
    grad_pre_gate = (grad_hid * pre_up * sig_gate * (1.0 + pre_gate * (1.0 - sig_gate))).astype(jnp.bfloat16)
    grad_pre_up = (grad_hid * silu_gate).astype(jnp.bfloat16)
    grad_gate = jnp.dot(exp_rows.T, grad_pre_gate, preferred_element_type=jnp.float32)
    grad_up = jnp.dot(exp_rows.T, grad_pre_up, preferred_element_type=jnp.float32)
    grad_rows = (jnp.dot(grad_pre_gate, gate_mat.T, preferred_element_type=jnp.float32) + jnp.dot(grad_pre_up, up_mat.T, preferred_element_type=jnp.float32)).astype(jnp.bfloat16)
    return exp_out, grad_rows, grad_gate, grad_up, grad_down


def reference(tok_in, expert_idx, gate_wt, w_gate, w_up, w_down, grad_out):
    pair_ids = expert_idx.reshape(GROUP_DEVS, TOKENS * TOP_K)
    expert_hits = (pair_ids[:, :, None] == jnp.arange(EXPERTS, dtype=jnp.int32)[None, None, :]).astype(jnp.int32)
    pair_slot = jnp.sum((jnp.cumsum(expert_hits, axis=1) - expert_hits) * expert_hits, axis=2)
    dev_ids = jnp.arange(GROUP_DEVS, dtype=jnp.int32)[:, None]
    flat_dest = jnp.where(pair_slot < CAPACITY, (pair_ids * GROUP_DEVS + dev_ids) * CAPACITY + pair_slot, TOTAL_ROWS).reshape(-1)
    tok_pairs = jnp.repeat(tok_in, TOP_K, axis=0)
    cot_pairs = (gate_wt.reshape(-1, 1) * jnp.repeat(grad_out, TOP_K, axis=0).astype(jnp.float32)).astype(jnp.bfloat16)
    row_buf = jnp.zeros((TOTAL_ROWS, HIDDEN), jnp.bfloat16).at[flat_dest].set(tok_pairs, mode="drop")
    cot_buf = jnp.zeros((TOTAL_ROWS, HIDDEN), jnp.bfloat16).at[flat_dest].set(cot_pairs, mode="drop")
    exp_out, grad_rows, grad_gate, grad_up, grad_down = lax.map(expert_step, (row_buf.reshape(EXPERTS, GROUP_DEVS * CAPACITY, HIDDEN), cot_buf.reshape(EXPERTS, GROUP_DEVS * CAPACITY, HIDDEN), w_gate, w_up, w_down))
    pair_out = jnp.take(exp_out.reshape(TOTAL_ROWS, HIDDEN), flat_dest, axis=0, mode="fill", fill_value=0).reshape(PART_TOKENS, TOP_K, HIDDEN)
    pair_grad = jnp.take(grad_rows.reshape(TOTAL_ROWS, HIDDEN), flat_dest, axis=0, mode="fill", fill_value=0).reshape(PART_TOKENS, TOP_K, HIDDEN)
    tok_out = (tok_in.astype(jnp.float32) + jnp.sum(gate_wt[:, :, None] * pair_out.astype(jnp.float32), axis=1)).astype(jnp.bfloat16)
    grad_in = (grad_out.astype(jnp.float32) + jnp.sum(pair_grad.astype(jnp.float32), axis=1)).astype(jnp.bfloat16)
    return tok_out, grad_in, grad_gate, grad_up, grad_down
```

```python
import functools

import jax
import jax.numpy as jnp
from jax import lax
from jax.experimental import pallas as pl
from jax.experimental.pallas import tpu as pltpu
from jax.sharding import PartitionSpec as P


BF = jnp.bfloat16
F32 = jnp.float32
ANY = pl.ANY

RELATION = ((0, 0), (0, 1), (1, 0), (1, 1), (-1, 0), (-1, 1), (2, 0), (2, 1))
BLK, WIN = 256, 272
CBLK, CWIN = 128, 144


def nn(lhs, rhs):
    return jnp.dot(lhs, rhs, preferred_element_type=F32)


def nt(lhs, rhs):
    return lax.dot_general(lhs, rhs, (((1,), (1,)), ((), ())), preferred_element_type=F32)


def tn(lhs, rhs):
    return lax.dot_general(lhs, rhs, (((0,), (0,)), ((), ())), preferred_element_type=F32)


def params():
    return pltpu.CompilerParams(vmem_limit_bytes=62 * 2**20, dimension_semantics=("arbitrary",))


def cost(flops, moved):
    return pl.CostEstimate(flops=int(flops), bytes_accessed=int(moved), transcendentals=0)


def route_kernel(capacity, idx_ref, gate_ref, eid_ref, out_ref, col_ref):
    n_exp, tokens = eid_ref.shape[0], idx_ref.shape[1]
    eid = eid_ref[...]
    hit = jnp.zeros((n_exp, tokens), F32)
    gate = jnp.zeros((n_exp, tokens), F32)
    for j in range(idx_ref.shape[0]):
        same = idx_ref[j:j + 1, :] == eid
        hit = jnp.where(same, 1.0, hit)
        gate = jnp.where(same, gate_ref[j:j + 1, :], gate)
    before = (lax.broadcasted_iota(jnp.int32, (128, 128), 0) < lax.broadcasted_iota(jnp.int32, (128, 128), 1)).astype(F32).astype(BF)
    seen = jnp.zeros((n_exp, 1), F32)
    for b in range(tokens // 128):
        h = hit[:, b * 128:(b + 1) * 128]
        slot = nn(h.astype(BF), before) + seen
        seen = seen + jnp.sum(h, axis=1, keepdims=True)
        pos = jnp.where((h > 0.0) & (slot < capacity), slot, -1.0)
        out_ref[:, 0, b * 128:(b + 1) * 128] = pos
        col_ref[b * 128:(b + 1) * 128, 0:n_exp] = pos.T
    out_ref[:, 1, :] = gate
    col_ref[:, n_exp:2 * n_exp] = gate.T


def route(idx_t, gate_t, eid, capacity):
    n_exp, tokens = eid.shape[0], idx_t.shape[1]
    return pl.pallas_call(
        functools.partial(route_kernel, capacity),
        out_shape=[jax.ShapeDtypeStruct((n_exp, 2, tokens), F32), jax.ShapeDtypeStruct((tokens, 2 * n_exp), F32)],
        cost_estimate=cost(20_000_000, 1_000_000), name="route",
    )(idx_t, gate_t, eid)


def choose(index, items, act):
    if len(items) == 1:
        act(items[0])
        return
    mid = len(items) // 2

    @pl.when(index < mid)
    def _():
        choose(index, items[:mid], act)

    @pl.when(index >= mid)
    def _():
        choose(index - mid, items[mid:], act)


def fetch_rows(tables, buf, sem, src, slot):
    def start(parts):
        row = 0
        for part in parts:
            pltpu.make_async_copy(part, buf.at[slot, pl.ds(row, part.shape[0])], sem.at[slot]).start()
            row += part.shape[0]

    choose(src, tables, start)


def await_rows(tables, buf, sem, slot):
    row = 0
    for part in tables[0]:
        pltpu.make_async_copy(part, buf.at[slot, pl.ds(row, part.shape[0])], sem.at[slot]).wait()
        row += part.shape[0]


def stage_rows(tables, buf, sem, source):
    step = pl.program_id(0)

    @pl.when(step == 0)
    def _():
        fetch_rows(tables, buf, sem, source(0), 0)

    @pl.when(step + 1 < pl.num_programs(0))
    def _():
        fetch_rows(tables, buf, sem, source(step + 1), (step + 1) % 2)

    await_rows(tables, buf, sem, step % 2)
    return step % 2


def gather_seats(posg_ref, base_ref, at, rows_ref, acc, gacc=None):
    acc[...] = jnp.zeros_like(acc)
    if gacc is not None:
        gacc[...] = jnp.zeros_like(gacc)
    iota = lax.broadcasted_iota(jnp.int32, (WIN, 1), 0).astype(F32)
    blocks = rows_ref.shape[0] // BLK
    for blk in range(blocks):
        base = pl.multiple_of(base_ref[at * blocks + blk], 8)
        cols = pl.ds(blk * BLK, BLK)
        hot = (posg_ref[0:1, cols] - base.astype(F32)) == iota
        win = pl.ds(base, WIN)
        acc[win, :] += nn(jnp.where(hot, 1.0, 0.0).astype(BF), rows_ref[cols, :])
        if gacc is not None:
            gacc[win, :] += jnp.sum(jnp.where(hot, posg_ref[1:2, cols], 0.0), axis=1, keepdims=True)


def split_refs(refs, sizes):
    out, at = [], 0
    for n in sizes:
        out.append(refs[at:at + n])
        at += n
    return out


def put(buf, slot, dests, sem, which):
    choose(which, dests, lambda dest: pltpu.make_async_copy(buf.at[slot], dest, sem.at[slot]).start())


def await_put(buf, slot, dests, sem):
    pltpu.make_async_copy(buf.at[slot], dests[0], sem.at[slot]).wait()


def fwd_kernel(sizes, n_w, n_skip, item, first_src, base_ref, *refs):
    n_tab, n_out = sum(sizes), len(sizes)
    tables = split_refs(refs[:n_tab], sizes)
    w_refs = refs[n_tab:n_tab + n_w]
    posg_ref = refs[n_tab + n_w + n_skip]
    rest = refs[n_tab + n_w + n_skip + 1:]
    outs = rest[:n_out]
    r_ref, h_ref, us_ref, buf, acc, ab, w, obuf, sem, osem, wsem = rest[n_out:]
    step, last = pl.program_id(0), pl.num_programs(0) - 1
    fp = h_ref.shape[1]
    n_loc = outs[0].shape[0]
    loc, src = item(step)
    w_at = loc if n_w > 1 else 0
    w_copies = [pltpu.make_async_copy(w_refs[i], w.at[i], wsem.at[i]) for i in range(n_w)]

    @pl.when(step == 0)
    def _():
        for copy in w_copies:
            copy.start()

    slot = stage_rows(tables, buf, sem, lambda s: item(s)[1] - first_src)
    gather_seats(posg_ref, base_ref, src * n_loc + loc, buf.at[slot], acc)
    r_ref[...] = acc[...].astype(BF)

    @pl.when(step == 0)
    def _():
        for copy in w_copies:
            copy.wait()

    @pl.when(step >= 2)
    def _():
        await_put(obuf, slot, [outs[0].at[0]], osem)

    ab[...] = nn(r_ref[...], w[w_at, :, :2 * fp])
    a = ab[:, :fp]
    b = ab[:, fp:]
    sg = jax.nn.sigmoid(a)
    silu = a * sg
    h_ref[...] = (silu * b).astype(BF)
    us_ref[:, :fp] = b * sg * (1.0 + a * (1.0 - sg))
    us_ref[:, fp:] = silu
    obuf[slot] = nt(h_ref[...], w[w_at, :, 2 * fp:]).astype(BF)
    put(obuf, slot, [out.at[loc] for out in outs], osem, src - first_src)

    @pl.when(step == last)
    def _():
        await_put(obuf, 1 - slot, [outs[0].at[0]], osem)
        await_put(obuf, slot, [outs[0].at[0]], osem)


def run_fwd(num, item, sources, base, tables, posg, ws, cap, outs=(), kept=()):
    n_src, n_loc, _, tokens = posg.shape
    width, wide = ws[0].shape
    fp = wide // 3
    any_spec = pl.BlockSpec(memory_space=ANY)
    tabs = tables[sources[0]:sources[1]]
    flat = [t for ts in tabs for t in ts]
    skip = (*outs, *kept)
    seat = lambda n: pl.BlockSpec((None, None, cap, n), lambda s, b: (*item(s), 0, 0))
    n_out = sources[1] - sources[0]
    n_in = 1 + len(flat) + len(ws)
    alias = {n_in + i: i for i in range(len(outs))} | {n_in + len(outs) + i: n_out + i for i in range(len(kept))}
    kept_shape = [jax.ShapeDtypeStruct((n_loc, n_src, cap, n), t) for n, t in ((width, BF), (fp, BF), (2 * fp, F32))]
    got = pl.pallas_call(
        functools.partial(fwd_kernel, tuple(len(ts) for ts in tabs), len(ws), len(skip), item, sources[0]),
        grid_spec=pltpu.PrefetchScalarGridSpec(
            num_scalar_prefetch=1, grid=(num,),
            in_specs=[any_spec] * (len(flat) + len(ws) + len(skip)) + [
                pl.BlockSpec((None, None, 2, tokens), lambda s, b: (*item(s)[::-1], 0, 0))],
            out_specs=[any_spec] * n_out + [seat(width), seat(fp), seat(2 * fp)],
            scratch_shapes=[pltpu.VMEM((2, tokens, width), BF), pltpu.VMEM((cap, width), F32), pltpu.VMEM((cap, 2 * fp), F32),
                            pltpu.VMEM((len(ws), width, wide), BF), pltpu.VMEM((2, cap, width), BF),
                            pltpu.SemaphoreType.DMA((2,)), pltpu.SemaphoreType.DMA((2,)), pltpu.SemaphoreType.DMA((len(ws),))]),
        out_shape=[jax.ShapeDtypeStruct((n_loc, cap, width), BF)] * n_out + kept_shape,
        input_output_aliases=alias,
        compiler_params=params(),
        cost_estimate=cost(2 * num * cap * width * wide, 12_000_000 * num),
    )(base, *flat, *ws, *skip, posg)
    return got[:n_out], got[n_out:]


def bwd_kernel(sizes, n_after, ffn, loc, n_loc, base_ref, *refs):
    n_tab, n_src = sum(sizes), len(sizes)
    tables = split_refs(refs[:n_tab], sizes)
    posg_ref, w_ref, r_ref, h_ref, us_ref = refs[n_tab + n_after:n_tab + n_after + 5]
    rest = refs[n_tab + n_after + 5:]
    outs = rest[:n_src]
    dw_ref, buf, gacc, dh, r2, c2, h2, dab2, dw, stage, obuf, sem, osem, rsem, dsem = rest[n_src:]
    step = pl.program_id(0)
    cap, fp = dh.shape
    width = c2.shape[1]
    rows = cap // 2
    slot = stage_rows(tables, buf, sem, lambda s: s)
    now = pl.multiple_of(slot * cap, cap)
    copies = [pltpu.make_async_copy(r_ref.at[loc, step], r2.at[pl.ds(now, cap)], rsem.at[0]),
              pltpu.make_async_copy(h_ref.at[loc, step], h2.at[pl.ds(now, cap)], rsem.at[1])]
    for copy in copies:
        copy.start()

    @pl.when(step == 0)
    def _():
        dw[...] = jnp.zeros_like(dw)

    gather_seats(posg_ref, base_ref, step * n_loc + loc, buf.at[slot], dh.at[:, pl.ds(0, width)], gacc)
    c2[pl.ds(now, cap), :] = (gacc[...] * dh[:, :width]).astype(BF)

    @pl.when(step >= 2)
    def _():
        await_put(obuf, slot, [outs[0].at[0]], osem)

    for half in range(2):
        part = pl.ds(half * rows, rows)
        here = pl.ds(pl.multiple_of(now + half * rows, rows), rows)
        dh[part, :] = nn(c2[here, :], w_ref[:, 2 * fp:])
        dab2[here, :fp] = (dh[part, :] * us_ref[part, :fp]).astype(BF)
        dab2[here, fp:] = (dh[part, :] * us_ref[part, fp:]).astype(BF)
        obuf[slot, part, :] = nt(dab2[here, :], w_ref[:, :2 * fp]).astype(BF)
    put(obuf, slot, [out.at[0] for out in outs], osem, step)
    for copy in copies:
        copy.wait()

    @pl.when(slot == 1)
    def _():
        dw[:, 2 * fp:] += tn(c2[...], h2[...])
        dw[:, :2 * fp] += tn(r2[...], dab2[...])

    @pl.when(step == n_src - 1)
    def _():
        await_put(obuf, 0, [outs[0].at[0]], osem)
        await_put(obuf, 1, [outs[0].at[0]], osem)
        flush = stage.shape[1]
        copies = []
        for i in range(3):
            for at_row in range(0, dw.shape[0], flush):
                use = len(copies) % 2
                if len(copies) >= 2:
                    copies[-2].wait()
                stage[use] = dw[at_row:at_row + flush, i * fp:i * fp + ffn]
                copies.append(pltpu.make_async_copy(stage.at[use], dw_ref.at[i, pl.ds(at_row, flush)], dsem.at[use]))
                copies[-1].start()
        for copy in copies[-2:]:
            copy.wait()


def run_bwd(loc, base, tables, posg, w, kept, cap, ffn, after=()):
    n_src, n_loc, _, tokens = posg.shape
    width, wide = w.shape
    fp = wide // 3
    flat = [t for ts in tables for t in ts]
    any_spec = pl.BlockSpec(memory_space=ANY)
    got = pl.pallas_call(
        functools.partial(bwd_kernel, tuple(len(ts) for ts in tables), len(after), ffn, loc, n_loc),
        grid_spec=pltpu.PrefetchScalarGridSpec(
            num_scalar_prefetch=1, grid=(n_src,),
            in_specs=[any_spec] * (len(flat) + len(after)) + [
                pl.BlockSpec((None, None, 2, tokens), lambda s, b: (s, loc, 0, 0)),
                pl.BlockSpec((width, wide), lambda s, b: (0, 0), pipeline_mode=pl.Buffered(1)),
                any_spec, any_spec,
                pl.BlockSpec((None, None, cap, 2 * fp), lambda s, b: (loc, s, 0, 0))],
            out_specs=[any_spec] * (n_src + 1),
            scratch_shapes=[pltpu.VMEM((2, tokens, width), BF), pltpu.VMEM((cap, 1), F32), pltpu.VMEM((cap, fp), F32),
                            pltpu.VMEM((2 * cap, width), BF), pltpu.VMEM((2 * cap, width), BF), pltpu.VMEM((2 * cap, fp), BF), pltpu.VMEM((2 * cap, 2 * fp), BF),
                            pltpu.VMEM((width, wide), F32), pltpu.VMEM((2, width // 6, ffn), F32), pltpu.VMEM((2, cap, width), BF),
                            pltpu.SemaphoreType.DMA((2,)), pltpu.SemaphoreType.DMA((2,)), pltpu.SemaphoreType.DMA((2,)), pltpu.SemaphoreType.DMA((2,))]),
        out_shape=[jax.ShapeDtypeStruct((1, cap, width), BF)] * n_src + [jax.ShapeDtypeStruct((3, width, ffn), F32)],
        compiler_params=pltpu.CompilerParams(vmem_limit_bytes=67_043_328, dimension_semantics=("arbitrary",)),
        cost_estimate=cost(4 * n_src * cap * width * wide, 12_000_000 * n_src),
    )(base, *flat, *after, posg, w, *kept)
    return got[:n_src], got[n_src]


def combine_kernel(cols, n_back, gated, n_after, per, base_ref, *refs):
    n = n_back
    back = refs[:n]
    start_ref, col_ref, out_ref, buf, sem = refs[n + n_after:]
    per_back, _, _ = back[0].shape
    step = pl.program_id(0)
    blocks = pl.num_programs(0) * per
    n_exp = col_ref.shape[1] // 2
    copies = [pltpu.make_async_copy(back[i], buf.at[pl.ds(i * per_back, per_back)], sem.at[i]) for i in range(n)]

    @pl.when(step == 0)
    def _():
        for copy in copies:
            copy.start()
        for copy in copies:
            copy.wait()

    iota = lax.broadcasted_iota(jnp.int32, (1, CWIN), 1).astype(F32)
    for b in range(per):
        rows_at = pl.ds(b * CBLK, CBLK)
        summed = None
        for i, col in enumerate(cols):
            base = pl.multiple_of(base_ref[col * blocks + step * per + b], 16)
            pick = jnp.where((col_ref[rows_at, col:col + 1] - base.astype(F32)) == iota, 1.0, 0.0).astype(BF)
            rows = nn(pick, buf[i, pl.ds(base, CWIN), :])
            if gated:
                rows = col_ref[rows_at, n_exp + col:n_exp + col + 1] * rows
            summed = rows if summed is None else summed + rows
        out_ref[rows_at, :] = (start_ref[rows_at, :].astype(F32) + summed).astype(out_ref.dtype)


def run_combine(back, cols, gated, start, col, base, dtype, after=(), per=4):
    _, cap, width = back[0].shape
    tokens, n = start.shape[0], len(back)
    spec = lambda w: pl.BlockSpec((per * CBLK, w), lambda s, b: (s, 0))
    any_spec = pl.BlockSpec(memory_space=ANY)
    return pl.pallas_call(
        functools.partial(combine_kernel, tuple(cols), n, gated, len(after), per),
        grid_spec=pltpu.PrefetchScalarGridSpec(
            num_scalar_prefetch=1, grid=(tokens // (per * CBLK),),
            in_specs=[any_spec] * (n + len(after)) + [spec(width), spec(col.shape[1])],
            out_specs=spec(width),
            scratch_shapes=[pltpu.VMEM((len(cols), cap, width), BF), pltpu.SemaphoreType.DMA((n,))]),
        out_shape=jax.ShapeDtypeStruct((tokens, width), dtype),
        compiler_params=params(), cost_estimate=cost(2 * len(cols) * tokens * 256 * width, 20_000_000),
    )(base, *back, *after, start, col)


def block_base(pos, block, window, cap, align):
    first = jnp.min(jnp.where(pos >= 0.0, pos, float(cap)).reshape(*pos.shape[:-1], -1, block), axis=-1)
    return (jnp.minimum(first.astype(jnp.int32), cap - window) // align * align).reshape(-1)


def solution(mesh):
    ep_size = mesh.shape["expert"]
    chips = ep_size // 2
    row_spec = P(("rep", "expert", "data"), None)
    wide_spec = P("expert", "data", None)
    down_spec = P("expert", None, "data")
    wide_out = P(("rep", "expert"), "data", None)
    down_out = P(("rep", "expert"), None, "data")

    def shift(v, steps, flip):
        return lax.ppermute(v, "expert", [(2 * c + k, 2 * ((c + steps) % chips) + (k ^ flip)) for c in range(chips) for k in range(2)])

    def tables(rows):
        half = rows.shape[0] // 2
        top, bottom = rows[:half], rows[half:]
        right_top, left_bottom = shift(top, 1, 0), shift(bottom, -1, 0)
        right_bottom, left_top = shift(bottom, 1, 0), shift(top, -1, 0)
        far = shift(right_top, 1, 0), shift(left_bottom, -1, 0)
        same = [(rows,), (right_top, right_bottom), (left_top, left_bottom), far]
        return [v for parts in same for v in (parts, tuple(shift(p, 0, 1) for p in parts))]

    def moe_step(tok_in, expert_idx, gate_wt, w_gate, w_up, w_down, grad_out):
        tokens, top_k = expert_idx.shape
        n_loc, _, ffn = w_gate.shape
        n_exp = n_loc * ep_size
        cap = (5 * top_k * tokens + 4 * n_exp - 1) // (4 * n_exp)
        n_src = len(RELATION)
        pad = (-ffn) % 128

        x_tabs = tables(tok_in)
        g_tabs = tables(grad_out)
        weights = []
        for e in range(n_loc):
            parts = [jnp.pad(v, ((0, 0), (0, pad))) for v in (w_gate[e], w_up[e], w_down[e].T)]
            packed = jnp.concatenate(parts, axis=1)
            weights.append(lax.all_gather(packed, "data", axis=0, tiled=True))

        me = lax.axis_index("expert")
        peers = jnp.stack([2 * ((me // 2 + s) % chips) + (me % 2 + f) % 2 for s, f in RELATION])
        eid = (peers[:, None] * n_loc + jnp.arange(n_loc)[None, :]).reshape(-1, 1).astype(jnp.int32)
        posg, col = route(expert_idx.T, gate_wt.T, eid, cap)
        home_base = block_base(posg[:, 0], CBLK, CWIN, cap, 16)
        posg = posg.reshape(n_src, n_loc, 2, tokens)
        moved = [posg[k] if k == 0 else shift(posg[k], *RELATION[k]) for k in range(n_src)]
        posg_in = jnp.stack(moved)
        base = block_base(posg_in[:, :, 0], BLK, WIN, cap, 8)

        def give_back(rows):
            return [rows[k] if k == 0 else shift(rows[k], -s, f) for k, (s, f) in enumerate(RELATION)]

        cut = n_src - 2
        outs, kept = run_fwd(cut, lambda s: (0, s), (0, cut), base, x_tabs, posg_in, weights[:1], cap)
        later = lambda s: (jnp.where(s < 2, 0, 1), jnp.where(s < 2, s + cut, s - 2))
        outs, kept = run_fwd(n_src + 2, later, (0, n_src), base, x_tabs, posg_in, weights, cap, outs, kept)
        back_o = give_back(outs)
        dr0, dw0 = run_bwd(0, base, g_tabs, posg_in, weights[0], kept, cap, ffn)
        back_d0 = give_back(dr0)
        g0 = lax.psum_scatter(dw0, "data", scatter_dimension=1, tiled=True)
        dr1, dw1 = run_bwd(1, base, g_tabs, posg_in, weights[1], kept, cap, ffn, after=(dw0,))
        back_d1 = give_back(dr1)
        g1 = lax.psum_scatter(dw1, "data", scatter_dimension=1, tiled=True)

        cols = [[k * n_loc + e for k in range(n_src)] for e in range(n_loc)]
        tok_out = run_combine(back_o, list(range(n_loc * n_src)), True, tok_in, col, home_base, BF, after=(dw1,))
        part = run_combine(back_d0, cols[0], False, grad_out, col, home_base, F32, after=(tok_out,))
        grad_in = run_combine(back_d1, cols[1], False, part, col, home_base, BF)
        grads = [jnp.stack([g0[i], g1[i]]) for i in range(3)]
        return tok_out, grad_in, grads[0], grads[1], jnp.swapaxes(grads[2], 1, 2)

    return jax.shard_map(moe_step, mesh=mesh, in_specs=(row_spec, row_spec, row_spec, wide_spec, wide_spec, down_spec, row_spec), out_specs=(row_spec, row_spec, wide_out, wide_out, down_out), check_vma=False)
```

```python
import functools

import jax
import jax.numpy as jnp
from jax import lax
from jax.experimental import pallas as pl
from jax.experimental.pallas import tpu as pltpu
from jax.sharding import PartitionSpec as P


BF = jnp.bfloat16
F32 = jnp.float32
ANY = pl.ANY

RELATION = ((0, 0), (0, 1), (1, 0), (1, 1), (-1, 0), (-1, 1), (2, 0), (2, 1))
BLK, WIN = 256, 272
CBLK, CWIN = 128, 144
EARLY = (2, 4)


def nn(lhs, rhs):
    return jnp.dot(lhs, rhs, preferred_element_type=F32)


def nt(lhs, rhs):
    return lax.dot_general(lhs, rhs, (((1,), (1,)), ((), ())), preferred_element_type=F32)


def tn(lhs, rhs):
    return lax.dot_general(lhs, rhs, (((0,), (0,)), ((), ())), preferred_element_type=F32)


def params():
    return pltpu.CompilerParams(vmem_limit_bytes=62 * 2**20, dimension_semantics=("arbitrary",))


def cost(flops, moved):
    return pl.CostEstimate(flops=int(flops), bytes_accessed=int(moved), transcendentals=0)


def route_kernel(capacity, idx_ref, gate_ref, eid_ref, out_ref, col_ref):
    n_exp, tokens = eid_ref.shape[0], idx_ref.shape[1]
    eid = eid_ref[...]
    hit = jnp.zeros((n_exp, tokens), F32)
    gate = jnp.zeros((n_exp, tokens), F32)
    for j in range(idx_ref.shape[0]):
        same = idx_ref[j:j + 1, :] == eid
        hit = jnp.where(same, 1.0, hit)
        gate = jnp.where(same, gate_ref[j:j + 1, :], gate)
    before = (lax.broadcasted_iota(jnp.int32, (128, 128), 0) < lax.broadcasted_iota(jnp.int32, (128, 128), 1)).astype(F32).astype(BF)
    seen = jnp.zeros((n_exp, 1), F32)
    for b in range(tokens // 128):
        h = hit[:, b * 128:(b + 1) * 128]
        slot = nn(h.astype(BF), before) + seen
        seen = seen + jnp.sum(h, axis=1, keepdims=True)
        pos = jnp.where((h > 0.0) & (slot < capacity), slot, -1.0)
        out_ref[:, 0, b * 128:(b + 1) * 128] = pos
        col_ref[b * 128:(b + 1) * 128, 0:n_exp] = pos.T
    out_ref[:, 1, :] = gate
    col_ref[:, n_exp:2 * n_exp] = gate.T


def route(idx_t, gate_t, eid, capacity):
    n_exp, tokens = eid.shape[0], idx_t.shape[1]
    return pl.pallas_call(
        functools.partial(route_kernel, capacity),
        out_shape=[jax.ShapeDtypeStruct((n_exp, 2, tokens), F32), jax.ShapeDtypeStruct((tokens, 2 * n_exp), F32)],
        cost_estimate=cost(20_000_000, 1_000_000), name="route",
    )(idx_t, gate_t, eid)


def choose(index, items, act):
    if len(items) == 1:
        act(items[0])
        return
    mid = len(items) // 2

    @pl.when(index < mid)
    def _():
        choose(index, items[:mid], act)

    @pl.when(index >= mid)
    def _():
        choose(index - mid, items[mid:], act)


def row_copies(parts, buf, sem, slot):
    row, copies = 0, []
    for part in parts:
        copies.append(pltpu.make_async_copy(part, buf.at[slot, pl.ds(row, part.shape[0])], sem.at[slot]))
        row += part.shape[0]
    return copies


def fetch_rows(tables, buf, sem, src, slot):
    def start(parts):
        for copy in row_copies(parts, buf, sem, slot):
            copy.start()

    choose(src, tables, start)


def stage_rows(tables, buf, sem, source, meanwhile):
    step = pl.program_id(0)

    @pl.when(step == 0)
    def _():
        fetch_rows(tables, buf, sem, source(0), 0)
        meanwhile()

    @pl.when(step + 1 < pl.num_programs(0))
    def _():
        fetch_rows(tables, buf, sem, source(step + 1), (step + 1) % 2)

    for copy in row_copies(tables[0], buf, sem, step % 2):
        copy.wait()
    return step % 2


def gather_seats(posg_ref, base_ref, at, rows_ref, acc, gacc=None):
    acc[...] = jnp.zeros_like(acc)
    if gacc is not None:
        gacc[...] = jnp.zeros_like(gacc)
    iota = lax.broadcasted_iota(jnp.int32, (WIN, 1), 0).astype(F32)
    blocks = rows_ref.shape[0] // BLK
    for blk in range(blocks):
        base = pl.multiple_of(base_ref[at * blocks + blk], 8)
        cols = pl.ds(blk * BLK, BLK)
        hot = (posg_ref[0:1, cols] - base.astype(F32)) == iota
        win = pl.ds(base, WIN)
        acc[win, :] += nn(jnp.where(hot, 1.0, 0.0).astype(BF), rows_ref[cols, :])
        if gacc is not None:
            gacc[win, :] += jnp.sum(jnp.where(hot, posg_ref[1:2, cols], 0.0), axis=1, keepdims=True)


def split_refs(refs, sizes):
    out, at = [], 0
    for n in sizes:
        out.append(refs[at:at + n])
        at += n
    return out


def put(buf, slot, dests, sem, which):
    choose(which, dests, lambda dest: pltpu.make_async_copy(buf.at[slot], dest, sem.at[slot]).start())


def await_put(buf, slot, dests, sem):
    pltpu.make_async_copy(buf.at[slot], dests[0], sem.at[slot]).wait()


def fwd_kernel(sizes, n_w, n_skip, n_loc, item, first_src, base_ref, *refs):
    n_tab, n_out = sum(sizes), len(sizes)
    tables = split_refs(refs[:n_tab], sizes)
    w_refs = refs[n_tab:n_tab + n_w]
    posg_ref = refs[n_tab + n_w + n_skip]
    rest = refs[n_tab + n_w + n_skip + 1:]
    outs = rest[:n_out]
    r_ref, h_ref, us_ref, buf, acc, ab, w, obuf, sem, osem, wsem = rest[n_out:]
    step, last = pl.program_id(0), pl.num_programs(0) - 1
    fp = h_ref.shape[1]
    loc, src = item(step)
    w_at = loc if n_w > 1 else 0
    w_copies = [pltpu.make_async_copy(w_refs[i], w.at[i], wsem.at[i]) for i in range(n_w)]

    def load_weights():
        for copy in w_copies:
            copy.start()

    slot = stage_rows(tables, buf, sem, lambda s: item(s)[1] - first_src, load_weights)
    gather_seats(posg_ref, base_ref, src * n_loc + loc, buf.at[slot], acc)
    r_ref[...] = acc[...].astype(BF)

    @pl.when(step == 0)
    def _():
        for copy in w_copies:
            copy.wait()

    @pl.when(step >= 2)
    def _():
        await_put(obuf, slot, [outs[0].at[0]], osem)

    ab[...] = nn(r_ref[...], w[w_at, :, :2 * fp])
    a = ab[:, :fp]
    b = ab[:, fp:]
    sg = jax.nn.sigmoid(a)
    silu = a * sg
    h_ref[...] = (silu * b).astype(BF)
    us_ref[:, :fp] = b * sg * (1.0 + a * (1.0 - sg))
    us_ref[:, fp:] = silu
    obuf[slot] = nt(h_ref[...], w[w_at, :, 2 * fp:]).astype(BF)
    put(obuf, slot, [out.at[jnp.minimum(loc, out.shape[0] - 1)] for out in outs], osem, src - first_src)

    @pl.when(step == last)
    def _():
        await_put(obuf, 1 - slot, [outs[0].at[0]], osem)
        await_put(obuf, slot, [outs[0].at[0]], osem)


def run_fwd(num, item, sources, base, tables, posg, ws, cap, outs=(), kept=()):
    n_src, n_loc, _, tokens = posg.shape
    width, wide = ws[0].shape
    fp = wide // 3
    any_spec = pl.BlockSpec(memory_space=ANY)
    tabs = tables[sources[0]:sources[1]]
    flat = [t for ts in tabs for t in ts]
    outs = outs or [None] * (sources[1] - sources[0])
    old = [i for i, v in enumerate(outs) if v is not None]
    skip = (*[outs[i] for i in old], *kept)
    seat = lambda n: pl.BlockSpec((None, None, cap, n), lambda s, b: (*item(s), 0, 0))
    n_out = sources[1] - sources[0]
    n_in = 1 + len(flat) + len(ws)
    alias = {n_in + j: i for j, i in enumerate(old)} | {n_in + len(old) + i: n_out + i for i in range(len(kept))}
    kept_shape = [jax.ShapeDtypeStruct((n_loc, n_src, cap, n), t) for n, t in ((width, BF), (fp, BF), (2 * fp, F32))]
    got = pl.pallas_call(
        functools.partial(fwd_kernel, tuple(len(ts) for ts in tabs), len(ws), len(skip), n_loc, item, sources[0]),
        grid_spec=pltpu.PrefetchScalarGridSpec(
            num_scalar_prefetch=1, grid=(num,),
            in_specs=[any_spec] * (len(flat) + len(ws) + len(skip)) + [
                pl.BlockSpec((None, None, 2, tokens), lambda s, b: (*item(s)[::-1], 0, 0))],
            out_specs=[any_spec] * n_out + [seat(width), seat(fp), seat(2 * fp)],
            scratch_shapes=[pltpu.VMEM((2, tokens, width), BF), pltpu.VMEM((cap, width), F32), pltpu.VMEM((cap, 2 * fp), F32),
                            pltpu.VMEM((len(ws), width, wide), BF), pltpu.VMEM((2, cap, width), BF),
                            pltpu.SemaphoreType.DMA((2,)), pltpu.SemaphoreType.DMA((2,)), pltpu.SemaphoreType.DMA((len(ws),))]),
        out_shape=[jax.ShapeDtypeStruct((1 if k in EARLY else n_loc, cap, width), BF) for k in range(*sources)] + kept_shape,
        input_output_aliases=alias,
        compiler_params=params(),
        cost_estimate=cost(2 * num * cap * width * wide, 12_000_000 * num),
    )(base, *flat, *ws, *skip, posg)
    return got[:n_out], got[n_out:]


def bwd_kernel(sizes, n_after, loc, n_loc, base_ref, *refs):
    n_tab, n_src = sum(sizes), len(sizes)
    tables = split_refs(refs[:n_tab], sizes)
    posg_ref, w_ref, r_ref, h_ref, us_ref = refs[n_tab + n_after:n_tab + n_after + 5]
    rest = refs[n_tab + n_after + 5:]
    outs = rest[:n_src]
    dw_ref, buf, gacc, dh, w, r2, c2, h2, dab2, dw, obuf, sem, osem, rsem, dsem = rest[n_src:]
    step = pl.program_id(0)
    cap, ffn = dh.shape
    fp = h2.shape[1]
    width = c2.shape[1]
    rows = cap // 2
    w_copy = pltpu.make_async_copy(w_ref, w, rsem.at[2])

    def meanwhile():
        w_copy.start()
        dw[...] = jnp.zeros_like(dw)
        for i in range(2):
            dab2[:, i * fp + ffn:(i + 1) * fp] = jnp.zeros((2 * cap, fp - ffn), BF)

    slot = stage_rows(tables, buf, sem, lambda s: s, meanwhile)
    now = pl.multiple_of(slot * cap, cap)
    copies = [pltpu.make_async_copy(r_ref.at[loc, step], r2.at[pl.ds(now, cap)], rsem.at[0]),
              pltpu.make_async_copy(h_ref.at[loc, step], h2.at[pl.ds(now, cap)], rsem.at[1])]
    for copy in copies:
        copy.start()
    gather_seats(posg_ref, base_ref, step * n_loc + loc, buf.at[slot], dh.at[:, pl.ds(0, width)], gacc)
    c2[pl.ds(now, cap), :] = (gacc[...] * dh[:, :width]).astype(BF)

    @pl.when(step == 0)
    def _():
        w_copy.wait()

    @pl.when(step >= 2)
    def _():
        await_put(obuf, slot, [outs[0].at[0]], osem)

    for half in range(2):
        part = pl.ds(half * rows, rows)
        here = pl.ds(pl.multiple_of(now + half * rows, rows), rows)
        dh[part, :] = nn(c2[here, :], w[:, 2 * fp:2 * fp + ffn])
        dab2[here, :ffn] = (dh[part, :] * us_ref[part, :ffn]).astype(BF)
        dab2[here, fp:fp + ffn] = (dh[part, :] * us_ref[part, fp:fp + ffn]).astype(BF)
        obuf[slot, part, :] = nt(dab2[here, :], w[:, :2 * fp]).astype(BF)
    put(obuf, slot, [out.at[0] for out in outs], osem, step)
    for copy in copies:
        copy.wait()

    @pl.when(slot == 1)
    def _():
        dw[:, 2 * fp:] += tn(c2[...], h2[...])
        dw[:, :2 * fp] += tn(r2[...], dab2[...])

    @pl.when(step == n_src - 1)
    def _():
        slots = dh.shape[0] // 128
        moves = []
        for i in range(3):
            for at_row in range(0, width, 128):
                use = pl.ds(len(moves) % slots * 128, 128)
                if len(moves) >= slots:
                    moves[-slots].wait()
                dh[use, :] = dw[at_row:at_row + 128, i * fp:i * fp + ffn]
                moves.append(pltpu.make_async_copy(dh.at[use], dw_ref.at[i, pl.ds(at_row, 128)], dsem.at[len(moves) % slots]))
                moves[-1].start()
        await_put(obuf, 0, [outs[0].at[0]], osem)
        await_put(obuf, 1, [outs[0].at[0]], osem)
        for move in moves[-slots:]:
            move.wait()


def run_bwd(loc, base, tables, posg, w, kept, cap, ffn, after=()):
    n_src, n_loc, _, tokens = posg.shape
    width, wide = w.shape
    fp = wide // 3
    flat = [t for ts in tables for t in ts]
    any_spec = pl.BlockSpec(memory_space=ANY)
    got = pl.pallas_call(
        functools.partial(bwd_kernel, tuple(len(ts) for ts in tables), len(after), loc, n_loc),
        grid_spec=pltpu.PrefetchScalarGridSpec(
            num_scalar_prefetch=1, grid=(n_src,),
            in_specs=[any_spec] * (len(flat) + len(after)) + [
                pl.BlockSpec((None, None, 2, tokens), lambda s, b: (s, loc, 0, 0)),
                any_spec, any_spec, any_spec,
                pl.BlockSpec((None, None, cap, 2 * fp), lambda s, b: (loc, s, 0, 0))],
            out_specs=[any_spec] * (n_src + 1),
            scratch_shapes=[pltpu.VMEM((2, tokens, width), BF), pltpu.VMEM((cap, 1), F32), pltpu.VMEM((cap, ffn), F32), pltpu.VMEM((width, wide), BF),
                            pltpu.VMEM((2 * cap, width), BF), pltpu.VMEM((2 * cap, width), BF), pltpu.VMEM((2 * cap, fp), BF), pltpu.VMEM((2 * cap, 2 * fp), BF),
                            pltpu.VMEM((width, wide), F32), pltpu.VMEM((2, cap, width), BF),
                            pltpu.SemaphoreType.DMA((2,)), pltpu.SemaphoreType.DMA((2,)), pltpu.SemaphoreType.DMA((3,)), pltpu.SemaphoreType.DMA((cap // 128,))]),
        out_shape=[jax.ShapeDtypeStruct((1, cap, width), BF)] * n_src + [jax.ShapeDtypeStruct((3, width, ffn), F32)],
        compiler_params=pltpu.CompilerParams(vmem_limit_bytes=67_043_328, dimension_semantics=("arbitrary",)),
        cost_estimate=cost(4 * n_src * cap * width * wide, 12_000_000 * n_src),
    )(base, *flat, *after, posg, w, *kept)
    return got[:n_src], got[n_src]


def combine_kernel(cols, n_back, gated, n_after, per, base_ref, *refs):
    n = n_back
    back = refs[:n]
    start_ref, col_ref, out_ref, buf, sem = refs[n + n_after:]
    starts = [sum(v.shape[0] for v in back[:i]) for i in range(n)]
    step = pl.program_id(0)
    blocks = pl.num_programs(0) * per
    n_exp = col_ref.shape[1] // 2
    copies = [pltpu.make_async_copy(back[i], buf.at[pl.ds(starts[i], back[i].shape[0])], sem.at[i]) for i in range(n)]

    @pl.when(step == 0)
    def _():
        for copy in copies:
            copy.start()
        for copy in copies:
            copy.wait()

    iota = lax.broadcasted_iota(jnp.int32, (1, CWIN), 1).astype(F32)
    for b in range(per):
        rows_at = pl.ds(b * CBLK, CBLK)
        summed = None
        for i, col in enumerate(cols):
            base = pl.multiple_of(base_ref[col * blocks + step * per + b], 16)
            pick = jnp.where((col_ref[rows_at, col:col + 1] - base.astype(F32)) == iota, 1.0, 0.0).astype(BF)
            rows = nn(pick, buf[i, pl.ds(base, CWIN), :])
            if gated:
                rows = col_ref[rows_at, n_exp + col:n_exp + col + 1] * rows
            summed = rows if summed is None else summed + rows
        out_ref[rows_at, :] = (start_ref[rows_at, :].astype(F32) + summed).astype(out_ref.dtype)


def run_combine(back, cols, gated, start, col, base, dtype, after=(), per=4):
    _, cap, width = back[0].shape
    tokens, n = start.shape[0], len(back)
    spec = lambda w: pl.BlockSpec((per * CBLK, w), lambda s, b: (s, 0))
    any_spec = pl.BlockSpec(memory_space=ANY)
    return pl.pallas_call(
        functools.partial(combine_kernel, tuple(cols), n, gated, len(after), per),
        grid_spec=pltpu.PrefetchScalarGridSpec(
            num_scalar_prefetch=1, grid=(tokens // (per * CBLK),),
            in_specs=[any_spec] * (n + len(after)) + [spec(width), spec(col.shape[1])],
            out_specs=spec(width),
            scratch_shapes=[pltpu.VMEM((len(cols), cap, width), BF), pltpu.SemaphoreType.DMA((n,))]),
        out_shape=jax.ShapeDtypeStruct((tokens, width), dtype),
        compiler_params=params(), cost_estimate=cost(2 * len(cols) * tokens * 256 * width, 20_000_000),
    )(base, *back, *after, start, col)


def block_base(pos, block, window, cap, align):
    first = jnp.min(jnp.where(pos >= 0.0, pos, float(cap)).reshape(*pos.shape[:-1], -1, block), axis=-1)
    return (jnp.minimum(first.astype(jnp.int32), cap - window) // align * align).reshape(-1)


def place_kernel(row, n_skip, g_ref, *refs):
    outs, (buf, sem_in, sem_out) = refs[n_skip:-3], refs[-3:]
    ins = [pltpu.make_async_copy(g_ref.at[i], buf.at[i], sem_in.at[i]) for i in range(len(outs))]
    puts = [pltpu.make_async_copy(buf.at[i], out.at[row], sem_out.at[i]) for i, out in enumerate(outs)]
    for copy in ins:
        copy.start()
    for copy, put_out in zip(ins, puts):
        copy.wait()
        put_out.start()
    for copy in puts:
        copy.wait()


def place(row, n_loc, g, into=()):
    n, rows, ffn = g.shape
    any_spec = pl.BlockSpec(memory_space=ANY)
    return pl.pallas_call(
        functools.partial(place_kernel, row, len(into)),
        in_specs=[any_spec] * (1 + len(into)), out_specs=[any_spec] * n,
        out_shape=[jax.ShapeDtypeStruct((n_loc, rows, ffn), F32)] * n,
        scratch_shapes=[pltpu.VMEM((n, rows, ffn), F32), pltpu.SemaphoreType.DMA((n,)), pltpu.SemaphoreType.DMA((n,))],
        input_output_aliases={1 + i: i for i in range(len(into))},
        cost_estimate=cost(1_000_000, 2 * n * rows * ffn * 4),
    )(g, *into)


def solution(mesh):
    ep_size = mesh.shape["expert"]
    chips = ep_size // 2
    row_spec = P(("rep", "expert", "data"), None)
    wide_spec = P("expert", "data", None)
    down_spec = P("expert", None, "data")
    wide_out = P(("rep", "expert"), "data", None)
    down_out = P(("rep", "expert"), None, "data")

    def shift(v, steps, flip):
        return lax.ppermute(v, "expert", [(2 * c + k, 2 * ((c + steps) % chips) + (k ^ flip)) for c in range(chips) for k in range(2)])

    def tables(rows):
        half = rows.shape[0] // 2
        top, bottom = rows[:half], rows[half:]
        right_top, left_bottom = shift(top, 1, 0), shift(bottom, -1, 0)
        right_bottom, left_top = shift(bottom, 1, 0), shift(top, -1, 0)
        far = shift(right_top, 1, 0), shift(left_bottom, -1, 0)
        same = [(rows,), (right_top, right_bottom), (left_top, left_bottom), far]
        return [v for parts in same for v in (parts, tuple(shift(p, 0, 1) for p in parts))]

    def moe_step(tok_in, expert_idx, gate_wt, w_gate, w_up, w_down, grad_out):
        tokens, top_k = expert_idx.shape
        n_loc, _, ffn = w_gate.shape
        n_exp = n_loc * ep_size
        cap = (5 * top_k * tokens + 4 * n_exp - 1) // (4 * n_exp)
        n_src = len(RELATION)
        pad = (-ffn) % 128

        x_tabs = tables(tok_in)
        g_tabs = tables(grad_out)
        weights = []
        for e in range(n_loc):
            parts = [jnp.pad(v, ((0, 0), (0, pad))) for v in (w_gate[e], w_up[e], w_down[e].T)]
            packed = jnp.concatenate(parts, axis=1)
            weights.append(lax.all_gather(packed, "data", axis=0, tiled=True))

        me = lax.axis_index("expert")
        peers = jnp.stack([2 * ((me // 2 + s) % chips) + (me % 2 + f) % 2 for s, f in RELATION])
        eid = (peers[:, None] * n_loc + jnp.arange(n_loc)[None, :]).reshape(-1, 1).astype(jnp.int32)
        posg, col = route(expert_idx.T, gate_wt.T, eid, cap)
        home_base = block_base(posg[:, 0], CBLK, CWIN, cap, 16)
        posg = posg.reshape(n_src, n_loc, 2, tokens)
        moved = [posg[k] if k == 0 else shift(posg[k], *RELATION[k]) for k in range(n_src)]
        posg_in = jnp.stack(moved)
        base = block_base(posg_in[:, :, 0], BLK, WIN, cap, 8)

        def give_back(rows, which=range(n_src)):
            return [v if k == 0 else shift(v, -RELATION[k][0], RELATION[k][1]) for k, v in zip(which, rows)]

        cut = n_src - 2
        outs, kept = run_fwd(cut, lambda s: (0, s), (0, cut), base, x_tabs, posg_in, weights[:1], cap)
        ahead = give_back([outs[k] for k in EARLY], EARLY)
        outs = [None if k in EARLY or k >= cut else outs[k] for k in range(n_src)]
        later = lambda s: (jnp.where(s < 2, 0, 1), jnp.where(s < 2, s + cut, s - 2))
        outs, kept = run_fwd(n_src + 2, later, (0, n_src), base, x_tabs, posg_in, weights, cap, outs, kept)
        back_o = give_back(outs)
        dr0, dw0 = run_bwd(0, base, g_tabs, posg_in, weights[0], kept, cap, ffn)
        back_d0 = give_back(dr0)
        g0 = lax.psum_scatter(dw0, "data", scatter_dimension=1, tiled=True)
        dr1, dw1 = run_bwd(1, base, g_tabs, posg_in, weights[1], kept, cap, ffn, after=(dw0,))
        back_d1 = give_back(dr1)
        g1 = lax.psum_scatter(dw1, "data", scatter_dimension=1, tiled=True)

        cols = [[k * n_loc + e for k in range(n_src)] for e in range(n_loc)]
        seats = [k * n_loc + e for k in range(n_src) for e in range(1 if k in EARLY else 0, n_loc)] + [k * n_loc for k in EARLY]
        tok_out = run_combine(back_o + ahead, seats, True, tok_in, col, home_base, BF, after=(dw1,))
        early = place(0, n_loc, g0)
        part = run_combine(back_d0, cols[0], False, grad_out, col, home_base, F32, after=(tok_out, early[0]))
        grad_in = run_combine(back_d1, cols[1], False, part, col, home_base, BF)
        grads = place(1, n_loc, g1, early)
        return tok_out, grad_in, grads[0], grads[1], jnp.swapaxes(grads[2], 1, 2)

    return jax.shard_map(moe_step, mesh=mesh, in_specs=(row_spec, row_spec, row_spec, wide_spec, wide_spec, down_spec, row_spec), out_specs=(row_spec, row_spec, wide_out, wide_out, down_out), check_vma=False)
```
